256 devices in a mesh: groups: 2 (over z), seq: 128 (over x, y, core).
Axes of the slice: x: 8, y: 8, z: 2, core: 2. Of those that a mesh axis runs over, the one named last changes fastest.
The devices are a block of a 8x8x16 slice.
Arguments:
- latents: bfloat16 [2048, 64, 640], P(('groups', 'seq')), parts along dimension 0, may hold values from -6 to 6
- norm_gain: float32 [640], replicated, may hold values from 0.25 to 1.75
- norm_bias: float32 [640], replicated, may hold values from -3 to 3
- conv_weight: bfloat16 [5760, 640], P('seq'), may hold values from -0.078125 to 0.078125
- time_weight: bfloat16 [320, 640], replicated, may hold values from -0.3125 to 0.3125
- first_gain: float32 [640], replicated, may hold values from 0.25 to 1.75
- tconv_weight: bfloat16 [1920, 640], P('seq'), may hold values from -0.125 to 0.125
- second_gain: float32 [640], replicated, may hold values from 0.25 to 1.75
- qkv_weight: bfloat16 [640, 1920], P('seq'), may hold values from -0.25 to 0.25
- out_weight: bfloat16 [640, 640], P('seq'), may hold values from -0.25 to 0.25
- timesteps: int32 [8], P('groups'), parts along dimension 0, may hold values from 0 to 999
Outputs:
- mixed: bfloat16 [2048, 64, 640], P(('groups', 'seq')), parts along dimension 0
The draws below stay inside these ranges and needn't reach their ends.
There are 2 independent parts, one for each index of `groups`. The reference program is written for one: setup_inputs(seed, part) draws one part's arguments, and reference() takes and returns one part's arrays. A program takes and returns all parts, laid end to end along the dimension named above; an argument that names none is the same for every part. Nothing has to cross between parts.
All inputs are finite; a program needn't handle non-finite values.
Results may differ from the reference program's by a relative error of at most 0.008.
Values may be sent and summed in bfloat16 or wider, within the bound.
A program may use at most 128 MiB of HBM per device.

```python
import jax
import jax.numpy as jnp
from jax import lax

C = 640
HEAD = 64
GROUPS = 32
TFEAT = 320
FRAMES = 16
W = 64
ROWS_DEV = 8
CLIPS = 4
SPLIT = 2
H = 16
IMAGES = 64


def set_ends(drawn, key, low, top_value):
    longest = drawn.shape.index(max(drawn.shape))
    spots = []
    for shift in (0, 1):
        where = [jax.random.randint(jax.random.fold_in(key, axis), (), 0, length) for axis, length in enumerate(drawn.shape)]
        where[longest] = (where[longest] + shift) % drawn.shape[longest]
        spots.append(tuple(where))
    return drawn.at[spots[0]].set(low).at[spots[1]].set(top_value)


def block_scale(stream_key, shape, split, low, top_value):
    loudness = 1.0
    for axis_at, blocks in split:
        steps = jax.random.uniform(jax.random.fold_in(jax.random.fold_in(stream_key, 6), axis_at), (blocks,), jnp.float32, low / len(split), top_value / len(split))
        loudness = loudness * jnp.repeat(jnp.exp(steps), shape[axis_at] // blocks).reshape((-1,) + (1,) * (len(shape) - 1 - axis_at))
    return loudness


def bell_draw(stream_key, dims, deviation, limit, shards=(), held_as=jnp.bfloat16):
    array = jax.random.normal(stream_key, dims, jnp.float32) * deviation
    if len(shards) > 0:
        array = block_scale(stream_key, dims, shards, -0.22, 0.18) * array
    return jnp.clip(array, min=-limit, max=limit).astype(held_as)


def setup_inputs(seed: int = 0, part: int = 0) -> dict:
    arg_keys = jax.random.split(jax.random.key(seed), 12)
    own_keys = jax.random.split(jax.random.fold_in(arg_keys[11], part), 12)
    return {
        "latents": bell_draw(own_keys[0], (IMAGES * H, W, C), 1.0, 6.0, ((0, 128),)),
        "norm_gain": jnp.clip(1.0 + 0.15 * jax.random.normal(arg_keys[1], (C,), jnp.float32), 0.25, 1.75),
        "norm_bias": bell_draw(arg_keys[2], (C,), 0.5, 3.0, (), jnp.float32),
        "conv_weight": bell_draw(arg_keys[3], (9 * C, C), (9 * C) ** -0.5, 0.078125, ((0, 128),)),
        "time_weight": bell_draw(arg_keys[4], (TFEAT, C), TFEAT ** -0.5, 0.3125),
        "first_gain": jnp.clip(1.0 + 0.15 * jax.random.normal(arg_keys[5], (C,), jnp.float32), 0.25, 1.75),
        "tconv_weight": bell_draw(arg_keys[6], (3 * C, C), (3 * C) ** -0.5, 0.125, ((0, 128),)),
        "second_gain": jnp.clip(1.0 + 0.15 * jax.random.normal(arg_keys[7], (C,), jnp.float32), 0.25, 1.75),
        "qkv_weight": bell_draw(arg_keys[8], (C, 3 * C), C ** -0.5, 0.25, ((0, 128),)),
        "out_weight": bell_draw(arg_keys[9], (C, C), C ** -0.5, 0.25, ((0, 128),)),
        "timesteps": set_ends(jax.random.randint(own_keys[10], (CLIPS,), 0, 1000), jax.random.fold_in(own_keys[10], 1), 0, 999).astype(jnp.int32),
    }


def time_embed(timesteps, time_weight):
    half = TFEAT // 2
    freqs = jnp.exp(-jnp.log(10000.0) * jnp.arange(half, dtype=jnp.float32) / half)
    angles = timesteps.astype(jnp.float32)[:, None] * freqs[None, :]
    feats = jnp.concatenate([jnp.cos(angles), jnp.sin(angles)], axis=-1)
    return jnp.dot(feats, time_weight.astype(jnp.float32), precision=lax.Precision.HIGHEST)

def layer_norm(values):
    mean = lax.optimization_barrier(jnp.mean(values, axis=-1, keepdims=True))
    centered = values - mean
    var = lax.optimization_barrier(jnp.mean(centered * centered, axis=-1, keepdims=True))
    return centered * lax.rsqrt(var + 1e-05)

def temporal_block(spatial, first_gain, tconv_weight, second_gain, qkv_weight, out_weight):
    clips, frames, places, chans = spatial.shape
    heads = chans // HEAD
    values = spatial.astype(jnp.float32)
    first = (layer_norm(values) * first_gain).astype(jnp.bfloat16)
    zero = jnp.zeros_like(first[:, :1])
    before = jnp.concatenate([zero, first[:, :-1]], axis=1)
    after = jnp.concatenate([first[:, 1:], zero], axis=1)
    stacked = jnp.concatenate([before, first, after], axis=-1).reshape(-1, 3 * chans)
    mid = values + jnp.dot(stacked, tconv_weight, preferred_element_type=jnp.float32).reshape(values.shape)
    second = (layer_norm(mid) * second_gain).astype(jnp.bfloat16)
    qkv = jnp.dot(second.reshape(-1, chans), qkv_weight, preferred_element_type=jnp.float32).astype(jnp.bfloat16)
    qkv = qkv.reshape(clips, frames, places, 3, heads, HEAD).astype(jnp.float32)
    query, key, value = (qkv[:, :, :, 0], qkv[:, :, :, 1], qkv[:, :, :, 2])
    scores = jnp.einsum('cfphd,cgphd->cphfg', query, key) * HEAD ** (-0.5)
    weights = jax.nn.softmax(scores, axis=-1).astype(jnp.bfloat16).astype(jnp.float32)
    attended = jnp.einsum('cphfg,cgphd->cfphd', weights, value).astype(jnp.bfloat16)
    projected = jnp.dot(attended.reshape(-1, chans), out_weight, preferred_element_type=jnp.float32)
    return (mid + projected.reshape(mid.shape)).astype(jnp.bfloat16)

def reference(latents, norm_gain, norm_bias, conv_weight, time_weight, first_gain, tconv_weight, second_gain, qkv_weight, out_weight, timesteps):
    images = CLIPS * FRAMES
    tiled = latents.reshape(SPLIT, images, ROWS_DEV, W, C)
    frames_in = jnp.transpose(tiled, (1, 0, 2, 3, 4)).reshape(images, H, W, C)
    temb = time_embed(timesteps, time_weight)
    temb_rows = temb[jnp.arange(images) // FRAMES]

    def spatial_one(inputs):
        image, bias_row = inputs
        values = image.astype(jnp.float32).reshape(H * W, GROUPS, C // GROUPS)
        mean = lax.optimization_barrier(jnp.mean(values, axis=(0, 2)))
        var = lax.optimization_barrier(jnp.mean(values * values, axis=(0, 2))) - mean * mean
        normed = (values - mean[None, :, None]) * lax.rsqrt(var + 1e-05)[None, :, None]
        normed = normed.reshape(H, W, C) * norm_gain + norm_bias
        normed = jax.nn.silu(normed).astype(jnp.bfloat16)
        padded = jnp.pad(normed, ((1, 1), (1, 1), (0, 0)))
        taps = [padded[dy:dy + H, dx:dx + W] for dy in range(3) for dx in range(3)]
        columns = jnp.concatenate(taps, axis=-1).reshape(H * W, 9 * C)
        conv = jnp.dot(columns, conv_weight, preferred_element_type=jnp.float32)
        return (image.reshape(H * W, C).astype(jnp.float32) + conv + bias_row[None, :]).astype(jnp.bfloat16)
    spatial = lax.map(spatial_one, (frames_in, temb_rows)).reshape(CLIPS, FRAMES, H * W, C)

    def temporal_one(clip_rows):
        return temporal_block(clip_rows[None], first_gain, tconv_weight, second_gain, qkv_weight, out_weight)[0]
    mixed = lax.map(temporal_one, spatial).reshape(images, SPLIT, ROWS_DEV, W, C)
    return jnp.transpose(mixed, (1, 0, 2, 3, 4)).reshape(images * H, W, C)
```

```python
import functools

import jax
import jax.numpy as jnp
from jax import lax
from jax.experimental import pallas as pl
from jax.experimental.pallas import tpu as pltpu
from jax.sharding import Mesh
from jax.sharding import PartitionSpec as P

HEAD = 64
GROUPS = 32
TFEAT = 320
FRAMES = 16
C = 640
RING = 8
ROWS = 512
HALF = 256
WIDTH = 64
SEQ = ("seq_0", "seq_1", "seq_2")
GROUPS_SEQ = ("groups", "seq_0", "seq_1", "seq_2")
F32 = jnp.float32
BF16 = jnp.bfloat16
MESH = pl.DeviceIdType.MESH
HIGHEST = lax.Precision.HIGHEST

SLOTS = ((0, 0), (0, 1), (0, 2), (0, 3), (0, 4), (1, 1), (1, 2), (1, 3))
UPWARD_LAST = (0, 1, 2, 3)
STEPS = 9


def wrap(i):
    return lax.rem(i + 2 * RING, RING)


def iota(shape, dim):
    return lax.broadcasted_iota(jnp.int32, shape, dim)


def kernel(
    lat,
    gain,
    bias,
    convw,
    timew,
    gain1,
    tconvw,
    gain2,
    qkvw,
    outw,
    steps,
    out,
    slots,
    raw,
    wconv,
    wt,
    wqkv,
    wo,
    patches,
    halo_out,
    halo_in,
    stat_out,
    stat_in,
    spatial,
    grouped,
    stacked,
    mid,
    attended,
    mixed,
    line_send,
    line_recv,
    plane_send,
    plane_recv,
    twin_send,
    twin_recv,
    pair_send,
    pair_recv,
    go_send,
    go_recv,
    back_send,
    back_recv,
):
    x, y, c = (lax.axis_index(name) for name in SEQ)
    a = x + c * (y - x)
    b = y + c * (x - y)
    me = 2 * y + c
    across = {"seq_0": wrap(x + 4), "seq_1": y, "seq_2": c}
    twin = {"seq_0": x, "seq_1": y, "seq_2": 1 - c}

    def core_mate(a2, b2):
        return {"seq_0": a2 + c * (b2 - a2), "seq_1": b2 + c * (a2 - b2), "seq_2": c}

    def row_mate(j):
        return {"seq_0": x, "seq_1": lax.div(j, 2), "seq_2": lax.rem(j, 2)}

    barrier = pltpu.get_barrier_semaphore()
    greeted = [row_mate(lax.rem(me + d, FRAMES)) for d in range(1, FRAMES)]
    greeted += [{"seq_0": wrap(x + d), "seq_1": y, "seq_2": c} for d in (1, -1, 4)]
    for other in greeted:
        pl.semaphore_signal(barrier, inc=1, device_id=other, device_id_type=MESH)

    raw[...] = jnp.zeros_like(raw)
    raw[0:45] = convw[...]
    raw[48:63] = tconvw[...]
    for k in range(3):
        raw[64 + 16 * k : 69 + 16 * k] = qkvw[:, C * k : C * (k + 1)]
    raw[112:117] = outw[...]
    device = FRAMES * x + me
    to, frm = iota((96, 128), 0), iota((96, 128), 1)
    shifted = lax.rem(45 * device, 48) + frm
    shifted = jnp.where(shifted >= 48, shifted - 48, shifted)
    hit = (frm < 45) & (shifted == to) & (to < 48)
    hit |= (frm >= 48) & (frm < 63) & (to >= 48) & (to < 64) & (((15 * device + frm - 48) & 15) == to - 48)
    for k in range(4):
        start, low = 64 + 16 * k, 64 + 16 * (k // 2)
        there = (5 * device + frm - start + 8 * (k % 2)) & 15
        hit |= (frm >= start) & (frm < start + 5) & (to >= low) & (to < low + 16) & (there == to - low)
    placed = jnp.dot(hit.astype(F32).astype(BF16), raw[...], preferred_element_type=F32).astype(BF16)
    slots[0, c, a, b] = placed[:48]
    slots[1, c, a, b] = placed[48:]

    sums, squares = jnp.zeros((1, C), F32), jnp.zeros((1, C), F32)
    for r in range(8):
        v = lat[WIDTH * r : WIDTH * (r + 1)].astype(F32)
        sums += jnp.sum(v, axis=0, keepdims=True)
        squares += jnp.sum(v * v, axis=0, keepdims=True)
    stat_row = iota((8, C), 0)
    stat_out[...] = jnp.where(stat_row == 0, sums, 0.0) + jnp.where(stat_row == 1, squares, 0.0)

    pl.semaphore_wait(barrier, len(greeted))

    sent = []

    def send(src, dst, send_sem, recv_sem, other):
        copy = pltpu.make_async_remote_copy(
            src_ref=src, dst_ref=dst, send_sem=send_sem, recv_sem=recv_sem, device_id=other, device_id_type=MESH
        )
        copy.start()
        sent.append(copy)

    def arrived(ref, sem):
        pltpu.make_async_copy(ref, ref, sem).wait()

    def slot_b(i):
        way, hops = SLOTS[i]
        return wrap(b + (hops if way else -hops))

    def along_line(part, i, way):
        hops = SLOTS[i][1] + 1
        ref = slots.at[part, c, a, slot_b(i)]
        n = (hops - 1) if way == 0 else (3 + hops)
        send(ref, ref, line_send.at[part, n], line_recv.at[part, n], core_mate(a, wrap(b + (-1 if way else 1))))

    def line_arrived(part, i):
        way, hops = SLOTS[i]
        n = (hops - 1) if way == 0 else (3 + hops)
        ref = slots.at[part, c, a, slot_b(i)]
        arrived(ref, line_recv.at[part, n])

    def block_a(way, k):
        return wrap(a + (k if way else -k))

    def along_plane(part, i, way, k):
        ref = slots.at[part, c, block_a(way, k - 1), slot_b(i)]
        sems = (plane_send.at[part, way, k - 1, i], plane_recv.at[part, way, k - 1, i])
        send(ref, ref, *sems, core_mate(wrap(a + (-1 if way else 1)), b))

    def plane_arrived(part, i, way, k):
        ref = slots.at[part, c, block_a(way, k), slot_b(i)]
        arrived(ref, plane_recv.at[part, way, k - 1, i])

    def to_twin(part, n, block):
        ref = slots.at[part, c, block]
        send(ref, ref, twin_send.at[part, n], twin_recv.at[part, n], twin)

    def ring_step(part, t):
        for i, (way, hops) in enumerate(SLOTS):
            k = t - hops + 1
            if k == 1:
                if i == 0:
                    along_line(part, 0, 0)
                    along_line(part, 0, 1)
                else:
                    line_arrived(part, i)
                    if hops < (3 if way else 4):
                        along_line(part, i, way)
                along_plane(part, i, 0, 1)
                along_plane(part, i, 1, 1)
            elif 2 <= k <= 4:
                for w in (0, 1):
                    plane_arrived(part, i, w, k - 1)
                    if k < 4 or (i in UPWARD_LAST) == (w == 0):
                        along_plane(part, i, w, k)
            elif k == 5:
                plane_arrived(part, i, 0 if i in UPWARD_LAST else 1, 4)
        if t == 4:
            to_twin(part, 0, a)
        elif t in (5, 6, 7):
            to_twin(part, 2 * (t - 4) - 1, block_a(0, t - 4))
            to_twin(part, 2 * (t - 4), block_a(1, t - 4))
        elif t == 8:
            to_twin(part, 7, block_a(0, 4))

    def twin_arrived(part):
        for n, far in enumerate((0, -1, 1, -2, 2, -3, 3, 4)):
            ref = slots.at[part, 1 - c, wrap(b + far)]
            arrived(ref, twin_recv.at[part, n])

    def step(s):
        if s < STEPS:
            ring_step(0, s)
        if 0 <= s - 5 < STEPS:
            ring_step(1, s - 5)

    step(0)
    send(stat_out, stat_in, pair_send.at[0], pair_recv.at[0], across)
    step(1)

    arrived(stat_in, pair_recv.at[0])
    member = (iota((C, 128), 0) >= 20 * iota((C, 128), 1)) & (iota((C, 128), 0) < 20 * iota((C, 128), 1) + 20)
    back = (iota((128, C), 1) >= 20 * iota((128, C), 0)) & (iota((128, C), 1) < 20 * iota((128, C), 0) + 20)
    totals = stat_out[...] + stat_in[...]
    entries = 2 * ROWS * (C // GROUPS)
    by_group = jnp.dot(totals, member.astype(F32), precision=HIGHEST, preferred_element_type=F32) / entries
    mean_g = by_group[0:1]
    rstd_g = lax.rsqrt(by_group[1:2] - mean_g * mean_g + 1e-05)
    row8 = iota((8, 128), 0)
    both = jnp.where(row8 == 0, mean_g, 0.0) + jnp.where(row8 == 1, rstd_g, 0.0)
    spread = jnp.dot(both, back.astype(F32), precision=HIGHEST, preferred_element_type=F32)
    scale = spread[1:2] * gain[...]
    offset = bias[...] - spread[0:1] * scale
    column = iota((WIDTH, C), 0)

    def with_shifts(v, at):
        patches[pl.ds(at, WIDTH), C : 2 * C] = v.astype(BF16)
        patches[pl.ds(at, WIDTH), 0:C] = jnp.where(column == 0, 0.0, pltpu.roll(v, 1, 0)).astype(BF16)
        after = jnp.where(column == WIDTH - 1, 0.0, pltpu.roll(v, WIDTH - 1, 0))
        patches[pl.ds(at, WIDTH), 2 * C : 3 * C] = after.astype(BF16)

    def norm_row(r, carry):
        at = pl.multiple_of(WIDTH * r, WIDTH)
        v = lat[pl.ds(at, WIDTH)].astype(F32) * scale + offset
        v = v / (1.0 + jnp.exp(-v))
        with_shifts(v, pl.multiple_of(at + WIDTH, WIDTH))
        return carry

    lax.fori_loop(0, 8, norm_row, 0)
    lower = lax.div(x, 4)
    edge = pl.multiple_of(ROWS - (ROWS - WIDTH) * lower, WIDTH)
    halo_out[...] = patches[pl.ds(edge, WIDTH), C : 2 * C]
    send(halo_out, halo_in, pair_send.at[1], pair_recv.at[1], across)
    step(2)

    clip = lax.rem(x, 4)
    t = steps[clip].astype(F32)
    freqs = jnp.exp(iota((8, TFEAT // 2), 1).astype(F32) * (-jnp.log(F32(10000.0)) / (TFEAT // 2)))
    angles = t * freqs
    half = TFEAT // 2
    temb = jnp.dot(jnp.cos(angles), timew[:half].astype(F32), precision=HIGHEST, preferred_element_type=F32)
    temb += jnp.dot(jnp.sin(angles), timew[half:].astype(F32), precision=HIGHEST, preferred_element_type=F32)
    temb = temb[0:1]

    arrived(halo_in, pair_recv.at[1])
    inner = pl.multiple_of((ROWS + WIDTH) * (1 - lower), WIDTH)
    outer = pl.multiple_of((ROWS + WIDTH) * lower, WIDTH)
    with_shifts(halo_in[...].astype(F32), inner)
    patches[pl.ds(outer, WIDTH), :] = jnp.zeros((WIDTH, 3 * C), BF16)

    for s in range(3, STEPS):
        step(s)
    twin_arrived(0)

    lane_row = iota((16, C), 0)

    def slot(part, j, xb, tile):
        y2 = j // 2
        at = (part, 0, xb, y2) if j % 2 == 0 else (part, 1, y2, xb)
        return slots[at + (slice(16 * tile, 16 * tile + 16),)]

    def tile_rows(part, each, row0, xb, tile, flip):
        rows = (lane_row ^ 8) if flip else lane_row
        first = row0 // each
        value = slot(part, first, xb, tile).astype(F32)
        for j in range(first + 1, (row0 + 15) // each + 1):
            value = jnp.where(rows >= each * j - row0, slot(part, j, xb, tile).astype(F32), value)
        if flip:
            value = jnp.concatenate([value[8:], value[:8]], axis=0)
        return value.astype(BF16)

    def conv_block(xb, carry):
        for n in range(45):
            at = pl.multiple_of(720 * xb + 16 * n, 16)
            wconv[pl.ds(at, 16)] = tile_rows(0, 45, 16 * n, xb, n % 3, False)
        return carry

    lax.fori_loop(0, RING, conv_block, 0)

    def conv_half(g, between):
        total = lat[HALF * g : HALF * (g + 1)].astype(F32) + temb
        for dy in range(3):
            total += jnp.dot(
                patches[HALF * g + WIDTH * dy : HALF * (g + 1) + WIDTH * dy],
                wconv[3 * C * dy : 3 * C * (dy + 1)],
                preferred_element_type=F32,
            )
            between(dy)
        spatial[HALF * g : HALF * (g + 1)] = total.astype(BF16)

    order = (8, 7, 9, 6, 10, 5, 11, 4, 12, 3, 13, 2, 14, 1, 15)

    def exchange(g):
        mine = pl.multiple_of(16 * me, 16)
        for d in order:
            j = lax.rem(me + d, FRAMES)
            src = spatial.at[pl.ds(pl.multiple_of(HALF * g + 16 * j, 16), 16)]
            send(src, grouped.at[g, pl.ds(mine, 16)], go_send.at[g, d], go_recv.at[g, d], row_mate(j))
        grouped[g, pl.ds(mine, 16)] = spatial[pl.ds(pl.multiple_of(HALF * g + mine, 16), 16)]

    conv_half(0, lambda dy: step(9 + dy) if dy < 2 else None)
    exchange(0)
    conv_half(1, lambda dy: step(11 + dy) if dy < 2 else None)
    exchange(1)
    step(13)
    twin_arrived(1)

    def rest_block(xb, carry):
        for n in range(15):
            at = pl.multiple_of(240 * xb + 16 * n, 16)
            wt[pl.ds(at, 16)] = tile_rows(1, 15, 16 * n, xb, 0, False)
        for n in range(5):
            at = pl.multiple_of(80 * xb + 16 * n, 16)
            wqkv[pl.ds(at, 16), 0:C] = tile_rows(1, 5, 16 * n, xb, 1, False)
            wqkv[pl.ds(at, 16), C : 2 * C] = tile_rows(1, 5, 16 * n, xb, 1, True)
            wqkv[pl.ds(at, 16), 2 * C :] = tile_rows(1, 5, 16 * n, xb, 2, False)
            wo[pl.ds(at, 16)] = tile_rows(1, 5, 16 * n, xb, 2, True)
        return carry

    lax.fori_loop(0, RING, rest_block, 0)

    def layer_norm(v):
        centered = v - jnp.sum(v, axis=-1, keepdims=True) * (1.0 / C)
        var = jnp.sum(centered * centered, axis=-1, keepdims=True) * (1.0 / C)
        return centered * lax.rsqrt(var + 1e-05)

    apart = (iota((16, HALF), 0) - iota((16, HALF), 1)) & 15
    mask = jnp.where(apart == 0, 0.0, -1e30).astype(F32)
    low_head = iota((HALF, 2 * HEAD), 1) < HEAD

    def temporal(g):
        values = grouped[g].astype(F32)
        first = (layer_norm(values) * gain1[...]).astype(BF16)
        stacked[0:16, 0:C] = jnp.zeros((16, C), BF16)
        stacked[16:HALF, 0:C] = first[: HALF - 16]
        stacked[:, C : 2 * C] = first
        stacked[0 : HALF - 16, 2 * C :] = first[16:]
        stacked[HALF - 16 :, 2 * C :] = jnp.zeros((16, C), BF16)
        mid[...] = values + jnp.dot(stacked[...], wt[...], preferred_element_type=F32)
        second = (layer_norm(mid[...]) * gain2[...]).astype(BF16)
        stacked[...] = jnp.dot(second, wqkv[...], preferred_element_type=F32).astype(BF16)
        for h in range(C // (2 * HEAD)):
            at = 2 * HEAD * h
            query = stacked[:, at : at + 2 * HEAD]
            key = stacked[:, C + at : C + at + 2 * HEAD]
            value = stacked[:, 2 * C + at : 2 * C + at + 2 * HEAD]
            wide = query.astype(F32)
            heads = [jnp.where(low_head, wide, 0.0), jnp.where(low_head, 0.0, wide)]
            both = jnp.concatenate(heads, axis=0).astype(BF16)
            scores = lax.dot_general(both, key, (((1,), (1,)), ((), ())), preferred_element_type=F32)
            scores = scores.reshape(2 * FRAMES, 16, HALF) * HEAD ** (-0.5) + mask[None]
            scores = scores.reshape(2 * HALF, HALF)
            top = jnp.max(scores, axis=-1, keepdims=True)
            expd = jnp.exp(scores - top)
            weights = (expd / jnp.sum(expd, axis=-1, keepdims=True)).astype(BF16)
            got = jnp.dot(weights, value, preferred_element_type=F32)
            attended[:, at : at + 2 * HEAD] = jnp.where(low_head, got[:HALF], got[HALF:]).astype(BF16)
        projected = jnp.dot(attended[...], wo[...], preferred_element_type=F32)
        mixed[g] = (mid[...] + projected).astype(BF16)

    def give_back(g):
        mine = pl.multiple_of(HALF * g + 16 * me, 16)
        for d in order:
            j = lax.rem(me + d, FRAMES)
            src = mixed.at[g, pl.ds(pl.multiple_of(16 * j, 16), 16)]
            send(src, out.at[pl.ds(mine, 16)], back_send.at[g, d], back_recv.at[g, d], row_mate(j))
        out[pl.ds(mine, 16)] = mixed[g, pl.ds(pl.multiple_of(16 * me, 16), 16)]

    for g in (0, 1):
        for d in order:
            j = lax.rem(me - d + FRAMES, FRAMES)
            arrived(grouped.at[g, pl.ds(pl.multiple_of(16 * j, 16), 16)], go_recv.at[g, d])
        temporal(g)
        give_back(g)
    for g in (0, 1):
        for d in order:
            j = lax.rem(me - d + FRAMES, FRAMES)
            arrived(out.at[pl.ds(pl.multiple_of(HALF * g + 16 * j, 16), 16)], back_recv.at[g, d])
    for copy in sent:
        copy.wait_send()


def shards(
    latents,
    norm_gain,
    norm_bias,
    conv_weight,
    time_weight,
    first_gain,
    tconv_weight,
    second_gain,
    qkv_weight,
    out_weight,
    timesteps,
):
    rows, width, chans = latents.shape
    vmem = pl.BlockSpec(memory_space=pltpu.VMEM)
    dma = pltpu.SemaphoreType.DMA
    result = pl.pallas_call(
        kernel,
        out_shape=jax.ShapeDtypeStruct((rows * width, chans), BF16),
        in_specs=[vmem] * 10 + [pl.BlockSpec(memory_space=pltpu.SMEM)],
        out_specs=vmem,
        scratch_shapes=[
            pltpu.VMEM((2, 2, RING, RING, 48, C), BF16),
            pltpu.VMEM((128, C), BF16),
            pltpu.VMEM((9 * C, C), BF16),
            pltpu.VMEM((3 * C, C), BF16),
            pltpu.VMEM((C, 3 * C), BF16),
            pltpu.VMEM((C, C), BF16),
            pltpu.VMEM((ROWS + 2 * WIDTH, 3 * C), BF16),
            pltpu.VMEM((WIDTH, C), BF16),
            pltpu.VMEM((WIDTH, C), BF16),
            pltpu.VMEM((8, C), F32),
            pltpu.VMEM((8, C), F32),
            pltpu.VMEM((ROWS, C), BF16),
            pltpu.VMEM((2, HALF, C), BF16),
            pltpu.VMEM((HALF, 3 * C), BF16),
            pltpu.VMEM((HALF, C), F32),
            pltpu.VMEM((HALF, C), BF16),
            pltpu.VMEM((2, HALF, C), BF16),
            dma((2, 7)),
            dma((2, 7)),
            dma((2, 2, 4, 8)),
            dma((2, 2, 4, 8)),
            dma((2, 8)),
            dma((2, 8)),
            dma((2,)),
            dma((2,)),
            dma((2, FRAMES)),
            dma((2, FRAMES)),
            dma((2, FRAMES)),
            dma((2, FRAMES)),
        ],
        compiler_params=pltpu.CompilerParams(
            collective_id=0, has_side_effects=True, vmem_limit_bytes=63 * 2**20
        ),
    )(
        latents.reshape(rows * width, chans),
        norm_gain.reshape(1, chans),
        norm_bias.reshape(1, chans),
        conv_weight,
        time_weight,
        first_gain.reshape(1, chans),
        tconv_weight,
        second_gain.reshape(1, chans),
        qkv_weight,
        out_weight,
        timesteps,
    )
    return result.reshape(rows, width, chans)


def solution(mesh):
    torus = Mesh(
        mesh.devices.reshape(mesh.shape["groups"], 8, 8, 2), ("groups", "seq_0", "seq_1", "seq_2")
    )
    return jax.shard_map(
        shards,
        mesh=torus,
        in_specs=(
            P(GROUPS_SEQ, None, None),
            P(),
            P(),
            P(SEQ, None),
            P(),
            P(),
            P(SEQ, None),
            P(),
            P(SEQ, None),
            P(SEQ, None),
            P("groups"),
        ),
        out_specs=P(GROUPS_SEQ, None, None),
        check_vma=False,
    )
```
